64 devices in a mesh: rep: 8 (over x, y, core), dp: 8 (over z).
Axes of the slice: x: 2, y: 2, z: 8, core: 2. Of those that a mesh axis runs over, the one named last changes fastest.
The devices are a block of a 4x4x8 slice.
Arguments:
- x: bfloat16 [64, 4096, 512], P(('rep', 'dp')), parts along dimension 0
- dy: bfloat16 [64, 4096, 512], P(('rep', 'dp')), parts along dimension 0
- w_gate: bfloat16 [2, 512, 1664], P(None, 'dp')
- w_up: bfloat16 [2, 512, 1664], P(None, 'dp')
- w_down: bfloat16 [2, 1664, 512], P(None, 'dp')
- m_w_gate: float32 [2, 512, 1664], P(None, 'dp')
- m_w_up: float32 [2, 512, 1664], P(None, 'dp')
- m_w_down: float32 [2, 1664, 512], P(None, 'dp')
- v_w_gate: float32 [2, 512, 1664], P(None, 'dp')
- v_w_up: float32 [2, 512, 1664], P(None, 'dp')
- v_w_down: float32 [2, 1664, 512], P(None, 'dp')
Outputs:
- output 1: bfloat16 [16, 512, 1664], P('rep', 'dp'), parts along dimension 0
- output 2: bfloat16 [16, 512, 1664], P('rep', 'dp'), parts along dimension 0
- output 3: bfloat16 [16, 1664, 512], P('rep', 'dp'), parts along dimension 0
- output 4: float32 [16, 512, 1664], P('rep', 'dp'), parts along dimension 0
- output 5: float32 [16, 512, 1664], P('rep', 'dp'), parts along dimension 0
- output 6: float32 [16, 1664, 512], P('rep', 'dp'), parts along dimension 0
- output 7: float32 [16, 512, 1664], P('rep', 'dp'), parts along dimension 0
- output 8: float32 [16, 512, 1664], P('rep', 'dp'), parts along dimension 0
- output 9: float32 [16, 1664, 512], P('rep', 'dp'), parts along dimension 0
There are 8 independent parts. The reference program is written for one: setup_inputs(seed, part) draws one part's arguments, and reference() takes and returns one part's arrays. A program takes and returns all parts, laid end to end along the dimension named above; an argument that names none is the same for every part.
All inputs are finite; a program needn't handle non-finite values.
Results may differ from the reference program's by a relative error of at most 0.0202.
Values are sent between devices in bfloat16 or wider.
A program may use at most 768 MiB of HBM per device.

```python
import jax
import jax.numpy as jnp
from jax import lax

SEQUENCES = 8
TOKENS = 4096
D = 512
FF = 1664
LAYERS = 2
NAMES = ("w_gate", "w_up", "w_down")
SHAPES = {"w_gate": (LAYERS, D, FF), "w_up": (LAYERS, D, FF), "w_down": (LAYERS, FF, D)}


def bump(key, n, height):
    away = (jnp.arange(n, dtype=jnp.int32) - jax.random.randint(key, (), 0, n, jnp.int32)) % n
    return jnp.where(away < n // 8, height, 1.0)


def together(key, own, strength):
    shared = jax.random.normal(key, own.shape[1:], jnp.float32)
    return (own + strength * shared) * lax.rsqrt(1 + strength * strength)


def setup_inputs(seed: int = 0, part: int = 0) -> dict:
    kx, kdy, ka, kb, kz, kf, kh, kl, *keys = jax.random.split(jax.random.key(seed), 8 + 3 * len(NAMES))
    kx, kdy, ka, kb = (jax.random.fold_in(k, part) for k in (kx, kdy, ka, kb))
    kw, km, kv = (keys[i::3] for i in range(3))
    shape = (SEQUENCES, TOKENS, D)
    much_x, much_dy = jax.random.uniform(kz, (2,), jnp.float32, 0.0, 1.0)
    loud = 2.0 ** jax.random.uniform(jax.random.fold_in(kz, 1), (), jnp.float32, -1.0, 2.0)
    layers = 2.0 ** jax.random.uniform(kl, (LAYERS, 1, 1), jnp.float32, -1.0, 1.0)
    x = together(ka, jax.random.normal(kx, shape, jnp.float32), much_x) * bump(kf, D, 4.0)
    dy = together(kb, jax.random.normal(kdy, shape, jnp.float32), much_dy)
    drawn = {"x": x.astype(jnp.bfloat16), "dy": (loud * dy * (SEQUENCES * TOKENS) ** -0.5).astype(jnp.bfloat16)}
    for key, name in zip(kw, NAMES, strict=True):
        w = jax.random.normal(key, SHAPES[name], jnp.float32) * SHAPES[name][1] ** -0.5
        drawn[name] = (w * {"w_gate": 1.0, "w_up": bump(kh, FF, 4.0), "w_down": layers}[name]).astype(jnp.bfloat16)
    for key, name in zip(km, NAMES, strict=True):
        drawn[f"m_{name}"] = 0.1 * jax.random.normal(key, SHAPES[name], jnp.float32)
    for key, name in zip(kv, NAMES, strict=True):
        drawn[f"v_{name}"] = jax.random.uniform(key, SHAPES[name], jnp.float32, 0.005, 0.015)
    return drawn


def matmul(a, w):
    return jnp.dot(a, w, preferred_element_type=jnp.float32).astype(jnp.bfloat16)


def normed(h):
    wide = h.astype(jnp.float32)
    scale = lax.rsqrt(jnp.mean(wide**2, -1, keepdims=True) + 1e-6)
    return (wide * scale).astype(jnp.bfloat16)


def layer(h, w):
    a = normed(h)
    gate = jnp.dot(a, w["w_gate"], preferred_element_type=jnp.float32)
    up = jnp.dot(a, w["w_up"], preferred_element_type=jnp.float32)
    return h + matmul((jax.nn.silu(gate) * up).astype(jnp.bfloat16), w["w_down"])


def adamw(w, m, v, g):
    m = 0.9 * m + 0.1 * g
    v = 0.95 * v + 0.05 * g * g
    step = m * lax.rsqrt(v + 1e-8) + 0.1 * w
    return (w - 0.02 * step).astype(jnp.bfloat16), m, v


def stack(weights, h):
    return lax.scan(lambda h, w: (layer(h, w), None), h, weights)[0]


def reference(x, dy, w_gate, w_up, w_down, m_w_gate, m_w_up, m_w_down, v_w_gate, v_w_up, v_w_down):
    weights = dict(zip(NAMES, (w_gate, w_up, w_down), strict=True))

    def take(so_far, sequence):
        h, by_y = sequence
        _, back = jax.vjp(lambda w: stack(w, h), weights)
        return jax.tree.map(lambda total, term: total + term.astype(jnp.float32), so_far, back(by_y)[0]), None

    none_yet = {name: jnp.zeros(w.shape, jnp.float32) for name, w in weights.items()}
    by_weights, _ = lax.scan(take, none_yet, (x, dy))
    gradients = [by_weights[name].astype(jnp.bfloat16).astype(jnp.float32) for name in NAMES]
    new = [
        adamw(w.astype(jnp.float32), m, v, g)
        for w, m, v, g in zip((w_gate, w_up, w_down), (m_w_gate, m_w_up, m_w_down), (v_w_gate, v_w_up, v_w_down), gradients, strict=True)
    ]
    return tuple(one[which] for which in range(3) for one in new)
```

```python
import functools

import jax
import jax.numpy as jnp
from jax import lax
from jax.experimental import pallas as pl
from jax.experimental.pallas import tpu as pltpu
from jax.sharding import PartitionSpec as P

BF16, F32 = jnp.bfloat16, jnp.float32
MESH = pl.DeviceIdType.MESH
TILE = 512
CHUNK = 256
GROUP = 2
VMEM_LIMIT = 63 * 1024 * 1024


def dot(a, b):
    return jnp.dot(a, b, preferred_element_type=F32)


def scale_of(wide):
    return lax.rsqrt(jnp.mean(wide * wide, -1, keepdims=True) + 1e-6)


def sigmoid(g):
    return 0.5 * jnp.tanh(0.5 * g) + 0.5


def adamw(w, m, v, g):
    m = 0.9 * m + 0.1 * g
    v = 0.95 * v + 0.05 * g * g
    step = m * lax.rsqrt(v + 1e-8) + 0.1 * w
    return (w - 0.02 * step).astype(BF16), m, v


def tile_rows(t):
    return pl.ds(pl.multiple_of(t * TILE, TILE), TILE)


def greet(others):
    barrier = pltpu.get_barrier_semaphore()
    for other in others:
        pl.semaphore_signal(barrier, inc=1, device_id=other, device_id_type=MESH)
    pl.semaphore_wait(barrier, len(others))


def forward_kernel(
    n, x_ref, gate_ref, up_ref, down_ref, h_ref, gu0_out, d0_out, gu1_out, d1_out,
    gu, dn, hid, own_sem, out_sem, send_sem, recv_sem, psend_sem, precv_sem,
):
    me = lax.axis_index("dp")
    rep = lax.axis_index("rep")
    core = lax.rem(rep, 2)
    right, left = {"dp": lax.rem(me + 1, n)}, {"dp": lax.rem(me + n - 1, n)}
    partner = {"rep": rep + 1 - 2 * core}
    layers, rows, ff = gate_ref.shape
    drows, d = down_ref.shape[1:]
    half, quarter = d // 2, d // 4

    def own(l):
        mine = pl.ds(pl.multiple_of(me * rows, rows), rows)
        down = pl.ds(pl.multiple_of(me * drows, 16), drows)
        return (
            pltpu.make_async_copy(gate_ref.at[l], gu.at[l, 0, mine], own_sem.at[l, 0]),
            pltpu.make_async_copy(up_ref.at[l], gu.at[l, 1, mine], own_sem.at[l, 1]),
            pltpu.make_async_copy(down_ref.at[l], dn.at[l, down], own_sem.at[l, 2]),
        )

    for l in range(layers):
        for copy in own(l):
            copy.start()
    greet((right, left, partner))

    def piece(l, c, side, part, k):
        if part == 0:
            start = pl.multiple_of(k * rows + side * (rows // 2), rows // 2)
            return gu.at[l, c, pl.ds(start, rows // 2)]
        start = pl.multiple_of(k * drows, 16)
        return dn.at[l, pl.ds(start, drows), pl.ds(pl.multiple_of(c * half + side * quarter, quarter), quarter)]

    def ring(l, side, part, s, k):
        ref = piece(l, core, side, part, k)
        return pltpu.make_async_remote_copy(
            ref, ref, send_sem.at[l, side, part, s], recv_sem.at[l, side, part, s], (right, left)[side], MESH
        )

    def across(l, c, side, part, s, k):
        ref = piece(l, c, side, part, k)
        return pltpu.make_async_remote_copy(
            ref, ref, psend_sem.at[l, side, part, s], precv_sem.at[l, side, part, s], partner, MESH
        )

    def holder(side, s):
        return lax.rem(me + n - s, n) if side == 0 else lax.rem(me + s, n)

    def gather_step(l, s):
        for part in range(2):
            for side in range(2):
                k = holder(side, s)

                @pl.when(s > 0)
                def _():
                    ring(l, side, part, s - 1, k).wait_recv()

                @pl.when(s < n - 1)
                def _():
                    ring(l, side, part, s, k).start()

                @pl.when(s > 0)
                def _():
                    across(l, core, side, part, s - 1, k).start()

    def gather_end(l):
        def body(s, _):
            for part in range(2):
                for side in range(2):
                    k = holder(side, s + 1)
                    across(l, 1 - core, side, part, s, k).wait_recv()
                    across(l, core, side, part, s, k).wait_send()
                    ring(l, side, part, s, holder(side, s)).wait_send()
            return 0

        lax.fori_loop(0, n - 1, body, 0)

    def outs(l):
        to = ((gu0_out, d0_out), (gu1_out, d1_out))[l]
        return (
            pltpu.make_async_copy(gu.at[l], to[0], out_sem.at[l, 0]),
            pltpu.make_async_copy(dn.at[l], to[1], out_sem.at[l, 1]),
        )

    for l in range(layers):
        for copy in own(l):
            copy.wait()

    def gather_first(s, _):
        gather_step(0, s)
        return 0

    lax.fori_loop(0, n, gather_first, 0)
    gather_step(1, jnp.int32(0))
    gather_end(0)
    for copy in outs(0):
        copy.start()

    def tile(t, _):
        @pl.when(t < n - 1)
        def _():
            gather_step(1, t + 1)

        x = x_ref[tile_rows(t), :].astype(F32)
        a = (x * scale_of(x)).astype(BF16)
        for c in range(0, ff, CHUNK):
            w = min(CHUNK, ff - c)
            if w == CHUNK:
                g = dot(a, gu[0, 0, :, c : c + w])
                u = dot(a, gu[0, 1, :, c : c + w])
            else:
                both = dot(a, jnp.concatenate([gu[0, 0, :, c : c + w], gu[0, 1, :, c : c + w]], 1))
                g, u = both[:, :w], both[:, w:]
            hid[:, c : c + w] = (g * sigmoid(g) * u).astype(BF16)
        y = dot(hid[...], dn[0]).astype(BF16)
        h_ref[tile_rows(t), :] = (x + y.astype(F32)).astype(BF16)
        return 0

    tiles = x_ref.shape[0] // TILE
    lax.fori_loop(0, tiles, tile, 0)

    def gather_rest(s, _):
        gather_step(1, s)
        return 0

    lax.fori_loop(min(tiles, n - 1) + 1, n, gather_rest, 0)
    gather_end(1)
    for copy in outs(1):
        copy.start()
    for l in range(layers):
        for copy in outs(l):
            copy.wait()


def forward(n, x, gate, up, down):
    tokens, d = x.shape
    layers, rows, ff = gate.shape
    drows = down.shape[1]
    gu, dn = jax.ShapeDtypeStruct((2, d, ff), BF16), jax.ShapeDtypeStruct((n * drows, d), BF16)
    any_, vmem = pl.BlockSpec(memory_space=pl.ANY), pl.BlockSpec(memory_space=pltpu.VMEM)
    sems = pltpu.SemaphoreType.DMA((layers, 2, 2, n - 1))
    return pl.pallas_call(
        functools.partial(forward_kernel, n),
        out_shape=(jax.ShapeDtypeStruct(x.shape, BF16), gu, dn, gu, dn),
        in_specs=[vmem, any_, any_, any_],
        out_specs=(vmem, any_, any_, any_, any_),
        scratch_shapes=[
            pltpu.VMEM((layers, 2, d, ff), BF16),
            pltpu.VMEM((layers, n * drows, d), BF16),
            pltpu.VMEM((TILE, ff), BF16),
            pltpu.SemaphoreType.DMA((layers, 3)),
            pltpu.SemaphoreType.DMA((layers, 2)),
            sems, sems, sems, sems,
        ],
        compiler_params=pltpu.CompilerParams(collective_id=0, has_side_effects=True, vmem_limit_bytes=VMEM_LIMIT),
        name="gather_forward",
    )(x, gate, up, down)


class Ring:
    def __init__(self, n, me, part, out, slots, send, recv):
        self.n, self.me, self.part, self.out, self.slots, self.send, self.recv = n, me, part, out, slots, send, recv

    def copy(self, side, src, s):
        to = lax.rem(self.me + (1 if side == 0 else self.n - 1), self.n)
        return pltpu.make_async_remote_copy(
            src, self.slots.at[side, s], self.send.at[side, s], self.recv.at[side, s], {"dp": to}, MESH
        )

    def owner(self, side, s):
        return lax.rem(self.me + 2 * self.n - 1 - s, self.n) if side == 0 else lax.rem(self.me + 1 + s, self.n)

    def step(self, s):
        n, slots = self.n, self.slots

        @pl.when(s == 0)
        def _():
            for side in range(2):
                self.copy(side, self.part(side, self.owner(side, s)), s).start()

        @pl.when(s > 0)
        def _():
            for side in range(2):
                here = slots.at[side, s - 1]
                self.copy(side, here, s - 1).wait_recv()
                total = here[...].astype(F32) + self.part(side, self.owner(side, s))[...].astype(F32)

                @pl.when(s < n - 1)
                def _():
                    here[...] = total.astype(BF16)
                    self.copy(side, here, s).start()

                @pl.when(s == n - 1)
                def _():
                    self.out(side)[...] = total.astype(BF16)

    def end(self):
        def body(s, _):
            for side in range(2):
                self.copy(side, self.slots.at[side, s], s).wait_send()
            return 0

        lax.fori_loop(0, self.n - 1, body, 0)


def gu_ring(n, me, part, out, bufs):
    rows = part.shape[1] // n
    return Ring(n, me, lambda side, k: part.at[side, pl.ds(pl.multiple_of(k * rows, rows), rows)], lambda side: out.at[side], *bufs)


def down_ring(n, me, part, out, bufs):
    rows, half = part.shape[0] // n, part.shape[1] // 2
    return Ring(
        n, me,
        lambda side, k: part.at[pl.ds(pl.multiple_of(k * rows, 16), rows), pl.ds(side * half, half)],
        lambda side: out.at[:, pl.ds(side * half, half)],
        *bufs,
    )


def ring_scratch(n, rows, columns):
    sems = pltpu.SemaphoreType.DMA((2, n - 1))
    return [pltpu.VMEM((2, n - 1, rows, columns), BF16), sems, sems]


def prepare(tokens, h_ref, dh_ref, a, a_t, dh_t):
    def body(t, _):
        rows = tile_rows(t)
        wide = h_ref[rows, :].astype(F32)
        normed = (wide * scale_of(wide)).astype(BF16)
        a[rows, :] = normed
        a_t[:, rows] = normed.T
        dh_t[:, rows] = dh_ref[rows, :].T
        return 0

    lax.fori_loop(0, tokens // TILE, body, 0)


def backward_chunk(tokens, c, w, refs, place, da, tick):
    dh_ref, gu, dn, a, a_t, dh_t, dn_t, gu_t, acc_g, acc_u, acc_d = refs
    units = pl.ds(c if isinstance(c, int) else pl.multiple_of(c, CHUNK), w)
    dn_t[:, :w] = dn[units, :].T
    if da is not None:
        gu_t[:w] = gu[0, :, units].T
        gu_t[w : 2 * w] = gu[1, :, units].T
    acc_g[...] = jnp.zeros_like(acc_g)
    acc_u[...] = jnp.zeros_like(acc_u)
    acc_d[...] = jnp.zeros_like(acc_d)

    def body(t, _):
        tick(t)
        rows = tile_rows(t)
        at = a[rows, :]
        if w == CHUNK:
            g = dot(at, gu[0, :, units])
            u = dot(at, gu[1, :, units])
        else:
            both = dot(at, jnp.concatenate([gu[0, :, units], gu[1, :, units]], 1))
            g, u = both[:, :w], both[:, w:]
        e = dot(dh_ref[rows, :], dn_t[:, :w]).astype(BF16).astype(F32)
        s = sigmoid(g)
        silu = g * s
        hid = (silu * u).astype(BF16)
        du = (e * silu).astype(BF16)
        dg = (e * u * (s + silu * (1.0 - s))).astype(BF16)
        acc_d[:, :w] += dot(dh_t[:, rows], hid)
        dgu = jnp.concatenate([dg, du], 1)
        if w == CHUNK:
            acc_g[...] += dot(a_t[:, rows], dg)
            acc_u[...] += dot(a_t[:, rows], du)
        else:
            acc_g[...] += dot(a_t[:, rows], dgu)
        if da is not None:
            da[rows, :] += dot(dgu, gu_t[: 2 * w, :])
        return 0

    lax.fori_loop(0, tokens // TILE, body, 0)
    if w == CHUNK:
        place(acc_g[...], acc_u[...], acc_d[...])
    else:
        place(acc_g[:, :w], acc_g[:, w : 2 * w], acc_d[:, :w])


def backward_layer(tokens, ff, refs, parts, part_d, da, tick):
    tiles = tokens // TILE
    first = 0
    for part in parts:
        columns = part.shape[2]

        def placed(c, w, base, part=part):
            def place(g, u, d):
                at = pl.ds(c - base if isinstance(c, int) else pl.multiple_of(c - base, CHUNK), w)
                part[0, :, at] = g.astype(BF16)
                part[1, :, at] = u.astype(BF16)
                part_d[pl.ds(c if isinstance(c, int) else pl.multiple_of(c, CHUNK), w), :] = d.astype(BF16).T

            return place

        whole = columns // CHUNK

        def chunk(j, _, base=first, placed=placed):
            backward_chunk(
                tokens, base + j * CHUNK, CHUNK, refs, placed(base + j * CHUNK, CHUNK, base), da,
                lambda t: tick((base // CHUNK + j) * tiles + t),
            )
            return 0

        lax.fori_loop(0, whole, chunk, 0)
        if columns % CHUNK:
            c = first + whole * CHUNK
            backward_chunk(tokens, c, columns % CHUNK, refs, placed(c, columns % CHUNK, first), da, lambda t, c=c: tick(c // CHUNK * tiles + t))
        first += columns


def at_ticks(k, first, every, ring, n):
    @pl.when((k >= first) & (k < first + n * every) & (lax.rem(k - first + every * 64, every) == 0))
    def _():
        ring.step((k - first) // every)


def last_kernel(n, h_ref, dh_ref, gu, dn, out_h, part_b, part_d, sum_a, a, a_t, dh_t, dn_t, gu_t, acc_g, acc_u, acc_d, da, part_a0, part_a1, *bufs):
    me = lax.axis_index("dp")
    tokens, d = h_ref.shape
    ff = dn.shape[0]
    greet(({"dp": lax.rem(me + 1, n)}, {"dp": lax.rem(me + n - 1, n)}))
    wide = part_a0.shape[2]
    rings = [
        gu_ring(n, me, part_a0, sum_a.at[:, :, pl.ds(0, wide)], bufs[0:3]),
        gu_ring(n, me, part_a1, sum_a.at[:, :, pl.ds(wide, wide)], bufs[3:6]),
    ]
    tiles = tokens // TILE

    def tick(k):
        at_ticks(k, GROUP * tiles, 4, rings[0], n)
        at_ticks(k, 2 * GROUP * tiles + 1, 3, rings[1], n)

    prepare(tokens, h_ref, dh_ref, a, a_t, dh_t)
    da[...] = jnp.zeros_like(da)
    refs = (dh_ref, gu, dn, a, a_t, dh_t, dn_t, gu_t, acc_g, acc_u, acc_d)
    backward_layer(tokens, ff, refs, (part_a0, part_a1, part_b), part_d, da, tick)
    for ring in rings:
        ring.end()

    def finish(t, _):
        rows = tile_rows(t)
        wide = h_ref[rows, :].astype(F32)
        r = scale_of(wide)
        by_a = da[rows, :].astype(BF16).astype(F32)
        by_h = by_a * r - wide * (r * r * r * jnp.mean(by_a * wide, -1, keepdims=True))
        out_h[rows, :] = (dh_ref[rows, :].astype(F32) + by_h.astype(BF16).astype(F32)).astype(BF16)
        return 0

    lax.fori_loop(0, tiles, finish, 0)


def first_kernel(
    n, h_ref, dh_ref, gu, dn, old_b, old_d, sum_old_b, sum_old_d, sum_a, sum_b, sum_d,
    a, a_t, dh_t, dn_t, acc_g, acc_u, acc_d, part_a0, part_a1, part_b, part_d, *bufs,
):
    me = lax.axis_index("dp")
    tokens, d = h_ref.shape
    ff = dn.shape[0]
    greet(({"dp": lax.rem(me + 1, n)}, {"dp": lax.rem(me + n - 1, n)}))
    wide = part_a0.shape[2]
    old = [down_ring(n, me, old_d, sum_old_d, bufs[0:3]), gu_ring(n, me, old_b, sum_old_b, bufs[3:6])]
    groups = [
        gu_ring(n, me, part_a0, sum_a.at[:, :, pl.ds(0, wide)], bufs[6:9]),
        gu_ring(n, me, part_a1, sum_a.at[:, :, pl.ds(wide, wide)], bufs[9:12]),
    ]
    tail = [down_ring(n, me, part_d, sum_d, bufs[12:15]), gu_ring(n, me, part_b, sum_b, bufs[15:18])]
    tiles = tokens // TILE

    def tick(k):
        at_ticks(k, 0, 4, old[0], n)
        at_ticks(k, 2, 4, old[1], n)
        at_ticks(k, GROUP * tiles + 1, 4, groups[0], n)
        at_ticks(k, 2 * GROUP * tiles, 3, groups[1], n)

    prepare(tokens, h_ref, dh_ref, a, a_t, dh_t)
    refs = (dh_ref, gu, dn, a, a_t, dh_t, dn_t, None, acc_g, acc_u, acc_d)
    backward_layer(tokens, ff, refs, (part_a0, part_a1, part_b), part_d, None, tick)

    def rest(s, _):
        for ring in tail:
            ring.step(s)
        return 0

    lax.fori_loop(0, n, rest, 0)
    for ring in old + groups + tail:
        ring.end()


def work_scratch(tokens, d):
    return [
        pltpu.VMEM((tokens, d), BF16),
        pltpu.VMEM((d, tokens), BF16),
        pltpu.VMEM((d, tokens), BF16),
        pltpu.VMEM((d, CHUNK), BF16),
    ]


def sums_scratch(d):
    return [pltpu.VMEM((d, CHUNK), F32)] * 3


def backward_last(n, h, dh, gu, dn):
    tokens, d = h.shape
    ff = dn.shape[0]
    wide, rest = GROUP * CHUNK, ff - 2 * GROUP * CHUNK
    vmem = pl.BlockSpec(memory_space=pltpu.VMEM)
    return pl.pallas_call(
        functools.partial(last_kernel, n),
        out_shape=(
            jax.ShapeDtypeStruct((tokens, d), BF16),
            jax.ShapeDtypeStruct((2, d, rest), BF16),
            jax.ShapeDtypeStruct((ff, d), BF16),
            jax.ShapeDtypeStruct((2, d // n, 2 * wide), BF16),
        ),
        in_specs=[vmem] * 4,
        out_specs=(vmem,) * 4,
        scratch_shapes=work_scratch(tokens, d)
        + [pltpu.VMEM((2 * CHUNK, d), BF16)]
        + sums_scratch(d)
        + [pltpu.VMEM((tokens, d), F32)]
        + [pltpu.VMEM((2, d, wide), BF16)] * 2
        + ring_scratch(n, d // n, wide)
        + ring_scratch(n, d // n, wide),
        compiler_params=pltpu.CompilerParams(collective_id=1, has_side_effects=True, vmem_limit_bytes=VMEM_LIMIT),
        name="layer1",
    )(h, dh, gu, dn)


def backward_first(n, h, dh, gu, dn, old_b, old_d):
    tokens, d = h.shape
    ff = dn.shape[0]
    wide, rest = GROUP * CHUNK, ff - 2 * GROUP * CHUNK
    vmem = pl.BlockSpec(memory_space=pltpu.VMEM)
    b, dd = jax.ShapeDtypeStruct((2, d // n, rest), BF16), jax.ShapeDtypeStruct((ff // n, d), BF16)
    return pl.pallas_call(
        functools.partial(first_kernel, n),
        out_shape=(b, dd, jax.ShapeDtypeStruct((2, d // n, 2 * wide), BF16), b, dd),
        in_specs=[vmem] * 6,
        out_specs=(vmem,) * 5,
        scratch_shapes=work_scratch(tokens, d)
        + sums_scratch(d)
        + [pltpu.VMEM((2, d, wide), BF16)] * 2
        + [pltpu.VMEM((2, d, rest), BF16), pltpu.VMEM((ff, d), BF16)]
        + ring_scratch(n, ff // n, d // 2)
        + ring_scratch(n, d // n, rest)
        + ring_scratch(n, d // n, wide)
        + ring_scratch(n, d // n, wide)
        + ring_scratch(n, ff // n, d // 2)
        + ring_scratch(n, d // n, rest),
        compiler_params=pltpu.CompilerParams(collective_id=2, has_side_effects=True, vmem_limit_bytes=VMEM_LIMIT),
        name="layer0",
    )(h, dh, gu, dn, old_b, old_d)


def solution(mesh):
    n = mesh.shape["dp"]

    def step(x, dy, *arrays):
        weights, m, v = (arrays[i : i + 3] for i in (0, 3, 6))
        h1, gu0, d0, gu1, d1 = forward(n, x[0], *weights)
        by_h1, part_b1, part_d1, sum_a1 = backward_last(n, h1, dy[0], gu1, d1)
        sum_b1, sum_d1, sum_a0, sum_b0, sum_d0 = backward_first(n, x[0], by_h1, gu0, d0, part_b1, part_d1)
        gu_sums = [jnp.concatenate(pair, -1) for pair in ((sum_a0, sum_b0), (sum_a1, sum_b1))]
        gradients = [jnp.stack([s[i] for s in gu_sums]).astype(F32) for i in range(2)]
        gradients.append(jnp.stack([sum_d0, sum_d1]).astype(F32))
        new = [adamw(w.astype(F32), m, v, g) for w, m, v, g in zip(weights, m, v, gradients, strict=True)]
        return tuple(one[which] for which in range(3) for one in new)

    states, cut = P(("rep", "dp"), None, None), P(None, "dp", None)
    return jax.shard_map(
        step,
        mesh=mesh,
        in_specs=(states, states) + (cut,) * 9,
        out_specs=(P("rep", "dp", None),) * 9,
        check_vma=False,
    )
```

```python
import functools

import jax
import jax.numpy as jnp
from jax import lax
from jax.experimental import pallas as pl
from jax.experimental.pallas import tpu as pltpu
from jax.sharding import PartitionSpec as P

BF16, F32 = jnp.bfloat16, jnp.float32
MESH = pl.DeviceIdType.MESH
TILE = 512
CHUNK = 256
PIECES = 4
EARLY = 5
VMEM_LIMIT = 63 * 1024 * 1024


def dot(a, b):
    return jnp.dot(a, b, preferred_element_type=F32)


def scale_of(wide):
    return lax.rsqrt(jnp.mean(wide * wide, -1, keepdims=True) + 1e-6)


def sigmoid(g):
    return 0.5 * jnp.tanh(0.5 * g) + 0.5


def adamw(w, m, v, g):
    m = 0.9 * m + 0.1 * g
    v = 0.95 * v + 0.05 * g * g
    step = m * lax.rsqrt(v + 1e-8) + 0.1 * w
    return (w - 0.02 * step).astype(BF16), m, v


def tile_rows(t):
    return pl.ds(pl.multiple_of(t * TILE, TILE), TILE)


def greet(others):
    barrier = pltpu.get_barrier_semaphore()
    for other in others:
        pl.semaphore_signal(barrier, inc=1, device_id=other, device_id_type=MESH)
    pl.semaphore_wait(barrier, len(others))


def forward_kernel(
    n, x_ref, gate_ref, up_ref, down_ref, h_ref, gu0_out, d0_out, gu1_out, d1_out,
    gu, dn, hid, own_sem, out_sem, send_sem, recv_sem, psend_sem, precv_sem,
):
    me = lax.axis_index("dp")
    rep = lax.axis_index("rep")
    core = lax.rem(rep, 2)
    right, left = {"dp": lax.rem(me + 1, n)}, {"dp": lax.rem(me + n - 1, n)}
    partner = {"rep": rep + 1 - 2 * core}
    layers, rows, ff = gate_ref.shape
    drows, d = down_ref.shape[1:]
    half, quarter = d // 2, d // 4
    tiles = x_ref.shape[0] // TILE

    def own(l):
        mine = pl.ds(pl.multiple_of(me * rows, rows), rows)
        down = pl.ds(pl.multiple_of(me * drows, 16), drows)
        return (
            pltpu.make_async_copy(gate_ref.at[l], gu.at[l, 0, mine], own_sem.at[l, 0]),
            pltpu.make_async_copy(up_ref.at[l], gu.at[l, 1, mine], own_sem.at[l, 1]),
            pltpu.make_async_copy(down_ref.at[l], dn.at[l, down], own_sem.at[l, 2]),
        )

    for l in range(layers):
        for copy in own(l):
            copy.start()
    greet((right, left, partner))

    def piece(l, c, part, k):
        if part < 2:
            start = pl.multiple_of(k * rows + part * (rows // 2), rows // 2)
            return gu.at[l, c, pl.ds(start, rows // 2)]
        start = pl.multiple_of(k * drows, 16)
        return dn.at[l, pl.ds(start, drows), pl.ds(pl.multiple_of(c * half + (part - 2) * quarter, quarter), quarter)]

    def hops(side, part):
        return n // 2 if side == part % 2 else n - 1 - n // 2

    def ring(l, side, part, s, k):
        ref = piece(l, core, part, k)
        return pltpu.make_async_remote_copy(
            ref, ref, send_sem.at[l, side, part, s], recv_sem.at[l, side, part, s], (right, left)[side], MESH
        )

    def across(l, c, side, part, s, k):
        ref = piece(l, c, part, k)
        return pltpu.make_async_remote_copy(
            ref, ref, psend_sem.at[l, side, part, s], precv_sem.at[l, side, part, s], partner, MESH
        )

    def holder(side, s):
        return lax.rem(me + n - s, n) if side == 0 else lax.rem(me + s, n)

    def gather_step(l, s):
        for part in range(PIECES):
            for side in range(2):
                k, last = holder(side, s), hops(side, part)

                @pl.when((s > 0) & (s <= last))
                def _():
                    ring(l, side, part, s - 1, k).wait_recv()

                @pl.when(s < last)
                def _():
                    ring(l, side, part, s, k).start()

                @pl.when((s > 0) & (s <= last))
                def _():
                    across(l, core, side, part, s - 1, k).start()

    def gather_end(l):
        def body(s, _):
            for part in range(PIECES):
                for side in range(2):

                    @pl.when(s < hops(side, part))
                    def _():
                        k = holder(side, s + 1)
                        across(l, 1 - core, side, part, s, k).wait_recv()
                        across(l, core, side, part, s, k).wait_send()
                        ring(l, side, part, s, holder(side, s)).wait_send()

            return 0

        lax.fori_loop(0, n // 2, body, 0)

    def outs(l):
        to = ((gu0_out, d0_out), (gu1_out, d1_out))[l]
        return (
            pltpu.make_async_copy(gu.at[l], to[0], out_sem.at[l, 0]),
            pltpu.make_async_copy(dn.at[l], to[1], out_sem.at[l, 1]),
        )

    for l in range(layers):
        for copy in own(l):
            copy.wait()

    def gather_first(s, _):
        gather_step(0, s)

        @pl.when(s == n // 4)
        def _():
            gather_step(1, s - n // 4)

        return 0

    lax.fori_loop(0, n // 2 + 1, gather_first, 0)
    gather_end(0)
    for copy in outs(0):
        copy.start()

    def tile(t, _):
        @pl.when(lax.rem(t * (n // 2), tiles) < n // 2)
        def _():
            gather_step(1, 1 + t * (n // 2) // tiles)

        x = x_ref[tile_rows(t), :].astype(F32)
        a = (x * scale_of(x)).astype(BF16)
        for c in range(0, ff, CHUNK):
            w = min(CHUNK, ff - c)
            if w == CHUNK:
                g = dot(a, gu[0, 0, :, c : c + w])
                u = dot(a, gu[0, 1, :, c : c + w])
            else:
                both = dot(a, jnp.concatenate([gu[0, 0, :, c : c + w], gu[0, 1, :, c : c + w]], 1))
                g, u = both[:, :w], both[:, w:]
            hid[:, c : c + w] = (g * sigmoid(g) * u).astype(BF16)
        y = dot(hid[...], dn[0]).astype(BF16)
        h_ref[tile_rows(t), :] = (x + y.astype(F32)).astype(BF16)
        return 0

    lax.fori_loop(0, tiles, tile, 0)
    gather_end(1)
    for copy in outs(1):
        copy.start()
    for l in range(layers):
        for copy in outs(l):
            copy.wait()


def forward(n, x, gate, up, down):
    tokens, d = x.shape
    layers, rows, ff = gate.shape
    drows = down.shape[1]
    gu, dn = jax.ShapeDtypeStruct((2, d, ff), BF16), jax.ShapeDtypeStruct((n * drows, d), BF16)
    any_, vmem = pl.BlockSpec(memory_space=pl.ANY), pl.BlockSpec(memory_space=pltpu.VMEM)
    sems = pltpu.SemaphoreType.DMA((layers, 2, PIECES, n // 2))
    return pl.pallas_call(
        functools.partial(forward_kernel, n),
        out_shape=(jax.ShapeDtypeStruct(x.shape, BF16), gu, dn, gu, dn),
        in_specs=[vmem, any_, any_, any_],
        out_specs=(vmem, any_, any_, any_, any_),
        scratch_shapes=[
            pltpu.VMEM((layers, 2, d, ff), BF16),
            pltpu.VMEM((layers, n * drows, d), BF16),
            pltpu.VMEM((TILE, ff), BF16),
            pltpu.SemaphoreType.DMA((layers, 3)),
            pltpu.SemaphoreType.DMA((layers, 2)),
            sems, sems, sems, sems,
        ],
        compiler_params=pltpu.CompilerParams(collective_id=0, has_side_effects=True, vmem_limit_bytes=VMEM_LIMIT),
        name="gather_forward",
    )(x, gate, up, down)


class Rings:
    def __init__(self, n, me, w, gu, dn, base, out_gu, out_dn, bufs):
        self.n, self.me, self.w, self.gu, self.dn, self.base, self.out_gu, self.out_dn = n, me, w, gu, dn, base, out_gu, out_dn
        self.bufs = (bufs[0:3], bufs[3:6])
        self.rows, self.half = gu.shape[1] // n, dn.shape[1] // 2
        self.far = n // 2
        self.actions = self.far + 1

    def hops(self, p, side):
        return self.far if side == p else self.n - 1 - self.far

    def part(self, kind, j, p, k):
        first = self.base + j * self.w
        if kind == 0:
            first = first if isinstance(first, int) else pl.multiple_of(first, self.w)
            return self.gu.at[p, pl.ds(pl.multiple_of(k * self.rows, self.rows), self.rows), pl.ds(first, self.w)]
        share = self.w // self.n
        return self.dn.at[pl.ds(pl.multiple_of(first + k * share, share), share), pl.ds(p * self.half, self.half)]

    def copy(self, kind, j, p, side, src, s):
        slots, send, recv = self.bufs[kind]
        at = s if side == 0 else self.hops(p, 0) + s
        to = lax.rem(self.me + (1 if side == 0 else self.n - 1), self.n)
        return pltpu.make_async_remote_copy(src, slots.at[j, p, at], send.at[j, p, at], recv.at[j, p, at], {"dp": to}, MESH)

    def slot(self, kind, j, p, side, s):
        return self.bufs[kind][0].at[j, p, s if side == 0 else self.hops(p, 0) + s]

    def step(self, j, s):
        n, me = self.n, self.me

        def whose(p, side, s):
            left = self.hops(p, side) - s
            return lax.rem(me + left, n) if side == 0 else lax.rem(me + n - left, n)

        every = [(kind, p, side) for kind in range(2) for p in range(2) for side in range(2)]

        @pl.when(s == 0)
        def _():
            for kind, p, side in every:
                self.copy(kind, j, p, side, self.part(kind, j, p, whose(p, side, 0)), 0).start()

        @pl.when((s > 0) & (s < self.far))
        def _():
            for kind, p, side in every:

                @pl.when(s < self.hops(p, side))
                def _():
                    here = self.slot(kind, j, p, side, s - 1)
                    self.copy(kind, j, p, side, here, s - 1).wait_recv()
                    term = self.part(kind, j, p, whose(p, side, s))[...]
                    here[...] = (here[...].astype(F32) + term.astype(F32)).astype(BF16)
                    self.copy(kind, j, p, side, here, s).start()

        @pl.when(s == self.far)
        def _():
            for kind in range(2):
                for p in range(2):
                    total = self.part(kind, j, p, me)[...].astype(F32)
                    for side in range(2):
                        here = self.slot(kind, j, p, side, self.hops(p, side) - 1)
                        self.copy(kind, j, p, side, here, self.hops(p, side) - 1).wait_recv()
                        total += here[...].astype(F32)
                    (self.out_gu(p, j) if kind == 0 else self.out_dn(p, j))[...] = total.astype(BF16)

    def end(self, count):
        def body(j, _):
            for kind in range(2):
                for p in range(2):
                    for side in range(2):
                        for s in range(self.hops(p, side)):
                            self.copy(kind, j, p, side, self.slot(kind, j, p, side, s), s).wait_send()
            return 0

        lax.fori_loop(0, count, body, 0)


def ring_scratch(n, count, w, d):
    sems = pltpu.SemaphoreType.DMA((count, 2, n - 1))
    return [
        pltpu.VMEM((count, 2, n - 1, d // n, w), BF16), sems, sems,
        pltpu.VMEM((count, 2, n - 1, w // n, d // 2), BF16), sems, sems,
    ]


def columns(ref, first, w):
    return lambda side, j: ref[side].at[:, pl.ds(first + j * w if isinstance(j, int) else pl.multiple_of(first + j * w, w), w)]


def shares(ref, first, n, w):
    half = ref.shape[1] // 2
    return lambda side, j: ref.at[pl.ds(pl.multiple_of(first + j * (w // n), w // n), w // n), pl.ds(side * half, half)]


def rotate3(rings, k, count, tiles):
    for more in (0, 3):
        j = lax.rem(2 * k + 2, 3) + more
        since = k - tiles * (j + 1)

        @pl.when((j < count) & (since >= 0) & (since < 3 * rings.actions))
        def _():
            rings.step(j, since // 3)


def rotate4(rings, k, count, tiles):
    for more in (0, 4):
        j = lax.rem(k, 4) + more
        since = k - tiles * (j + 1) - lax.rem(k, 4)

        @pl.when((j < count) & (since >= 0) & (since < 4 * rings.actions))
        def _():
            rings.step(j, since // 4)


class Handover:
    def __init__(self, n, me, ff, summed, to, send, recv):
        self.n, self.me, self.summed, self.to, self.send, self.recv = n, me, summed, to, send, recv
        self.units, self.per = ff // 16 // n, CHUNK // n // 16
        self.whole = ff // CHUNK * (CHUNK // 16)

    def copy(self, i):
        n, me, per = self.n, self.me, self.per
        whole = ff_unit = (i // per) * (n * per) + me * per + i % per
        if i * n * 16 >= self.whole * 16:
            left = self.units - self.whole // n
            ff_unit = self.whole + me * left + (i - self.whole // n)
        del whole
        owner, slot = ff_unit // self.units, lax.rem(ff_unit, self.units)
        src, dst = self.summed.at[pl.ds(16 * i, 16)], self.to.at[slot]
        return owner, slot, pltpu.make_async_remote_copy(src, dst, self.send.at[i], self.recv.at[slot], {"dp": owner}, MESH)

    def start(self):
        for i in range(self.units):
            owner, slot, copy = self.copy(i)

            @pl.when(owner == self.me)
            def _():
                self.to[slot] = self.summed[16 * i : 16 * i + 16, :]

            @pl.when(owner != self.me)
            def _():
                copy.start()

    def end(self):
        for i in range(self.units):
            owner, _, copy = self.copy(i)

            @pl.when(owner != self.me)
            def _():
                copy.wait_send()

        def body(slot, _):
            unit = self.units * self.me + slot
            left = self.units - self.whole // self.n
            source = jnp.where(unit < self.whole, lax.rem(unit, self.n * self.per) // self.per, (unit - self.whole) // left)

            @pl.when(source != self.me)
            def _():
                ref = self.to.at[slot]
                pltpu.make_async_remote_copy(ref, ref, self.send.at[0], self.recv.at[slot], {"dp": source}, MESH).wait_recv()

            return 0

        lax.fori_loop(0, self.units, body, 0)


def prepare(tokens, h_ref, dh_ref, a, a_t, dh_t):
    def body(t, _):
        rows = tile_rows(t)
        wide = h_ref[rows, :].astype(F32)
        normed = (wide * scale_of(wide)).astype(BF16)
        a[rows, :] = normed
        a_t[:, rows] = normed.T
        dh_t[:, rows] = dh_ref[rows, :].T
        return 0

    lax.fori_loop(0, tokens // TILE, body, 0)


def backward_chunk(tokens, c, w, refs, place, da, tick):
    dh_ref, gu, dn, a, a_t, dh_t, dn_t, gu_t, acc_g, acc_u, acc_d = refs
    units = pl.ds(c if isinstance(c, int) else pl.multiple_of(c, CHUNK), w)
    dn_t[:, :w] = dn[units, :].T
    if da is not None:
        gu_t[:w] = gu[0, :, units].T
        gu_t[w : 2 * w] = gu[1, :, units].T
    acc_g[...] = jnp.zeros_like(acc_g)
    acc_u[...] = jnp.zeros_like(acc_u)
    acc_d[...] = jnp.zeros_like(acc_d)

    def body(t, _):
        tick(t)
        rows = tile_rows(t)
        at = a[rows, :]
        if w == CHUNK:
            g = dot(at, gu[0, :, units])
            u = dot(at, gu[1, :, units])
        else:
            both = dot(at, jnp.concatenate([gu[0, :, units], gu[1, :, units]], 1))
            g, u = both[:, :w], both[:, w:]
        e = dot(dh_ref[rows, :], dn_t[:, :w]).astype(BF16).astype(F32)
        s = sigmoid(g)
        silu = g * s
        hid = (silu * u).astype(BF16)
        du = (e * silu).astype(BF16)
        dg = (e * u * (s + silu * (1.0 - s))).astype(BF16)
        acc_d[:, :w] += dot(dh_t[:, rows], hid)
        dgu = jnp.concatenate([dg, du], 1)
        if w == CHUNK:
            acc_g[...] += dot(a_t[:, rows], dg)
            acc_u[...] += dot(a_t[:, rows], du)
        else:
            acc_g[...] += dot(a_t[:, rows], dgu)
        if da is not None:
            da[rows, :] += dot(dgu, gu_t[: 2 * w, :])
        return 0

    lax.fori_loop(0, tokens // TILE, body, 0)
    if w == CHUNK:
        place(acc_g[...], acc_u[...], acc_d[...])
    else:
        place(acc_g[:, :w], acc_g[:, w : 2 * w], acc_d[:, :w])


def backward_layer(tokens, refs, place, ff, da, tick):
    tiles = tokens // TILE
    whole = ff // CHUNK

    def chunk(j, _):
        c = pl.multiple_of(j * CHUNK, CHUNK)
        backward_chunk(tokens, c, CHUNK, refs, place(c, CHUNK), da, lambda t: tick(j * tiles + t))
        return 0

    lax.fori_loop(0, whole, chunk, 0)
    if ff % CHUNK:
        backward_chunk(tokens, whole * CHUNK, ff % CHUNK, refs, place(whole * CHUNK, ff % CHUNK), da, lambda t: tick(whole * tiles + t))


def placer(gu_part, dn_part):
    def place(c, w):
        def put(g, u, d):
            gu_part[0, :, pl.ds(c, w)] = g.astype(BF16)
            gu_part[1, :, pl.ds(c, w)] = u.astype(BF16)
            dn_part[pl.ds(c, w), :] = d.astype(BF16).T

        return put

    return place


def last_kernel(
    n, early, h_ref, dh_ref, gu, dn, out_h, out_gu, out_dn, sum_g, sum_u, sum_d,
    a, a_t, dh_t, dn_t, gu_t, acc_g, acc_u, acc_d, da, gu_part, dn_part, *bufs,
):
    me = lax.axis_index("dp")
    tokens, d = h_ref.shape
    ff = dn.shape[0]
    greet(({"dp": lax.rem(me + 1, n)}, {"dp": lax.rem(me + n - 1, n)}))
    rings = Rings(n, me, CHUNK, gu_part, dn_part, 0, columns((sum_g, sum_u), 0, CHUNK), shares(sum_d, 0, n, CHUNK), bufs)
    tiles = tokens // TILE
    prepare(tokens, h_ref, dh_ref, a, a_t, dh_t)
    da[...] = jnp.zeros_like(da)
    refs = (dh_ref, gu, dn, a, a_t, dh_t, dn_t, gu_t, acc_g, acc_u, acc_d)
    backward_layer(tokens, refs, placer(gu_part, dn_part), ff, da, lambda k: rotate3(rings, k, early, tiles))
    out_gu[...] = gu_part[:, :, early * CHUNK :]
    out_dn[...] = dn_part[early * CHUNK :, :]

    def finish(t, _):
        rows = tile_rows(t)
        wide = h_ref[rows, :].astype(F32)
        r = scale_of(wide)
        by_a = da[rows, :].astype(BF16).astype(F32)
        by_h = by_a * r - wide * (r * r * r * jnp.mean(by_a * wide, -1, keepdims=True))
        out_h[rows, :] = (dh_ref[rows, :].astype(F32) + by_h.astype(BF16).astype(F32)).astype(BF16)
        return 0

    lax.fori_loop(0, tiles, finish, 0)
    rings.end(early)


def first_kernel(
    n, early, h_ref, dh_ref, gu, dn, old_gu, old_dn, old_sum_g, old_sum_u, old_sum_d, sum_g, sum_u, sum_d,
    a, a_t, dh_t, dn_t, acc_g, acc_u, acc_d, gu_part, dn_part, summed, old_summed, send, recv, old_send, old_recv, *bufs,
):
    me = lax.axis_index("dp")
    tokens, d = h_ref.shape
    ff = dn.shape[0]
    whole, left = ff // CHUNK, ff % CHUNK
    share = CHUNK // n
    barrier = pltpu.get_barrier_semaphore()
    for other in range(1, n):
        pl.semaphore_signal(barrier, inc=1, device_id={"dp": lax.rem(me + other, n)}, device_id_type=MESH)
    pl.semaphore_wait(barrier, n - 1)
    old_g, old_u, new_g, new_u = sum_g.at[1], sum_u.at[1], sum_g.at[0], sum_u.at[0]
    old = Rings(
        n, me, CHUNK, old_gu, old_dn, 0, columns((old_g, old_u), early * CHUNK, CHUNK), shares(old_summed, early * share, n, CHUNK), bufs[0:6]
    )
    old_left = Rings(
        n, me, left, old_gu, old_dn, (whole - early) * CHUNK, columns((old_g, old_u), whole * CHUNK, left), shares(old_summed, whole * share, n, left), bufs[6:12]
    )
    new = Rings(n, me, CHUNK, gu_part, dn_part, 0, columns((new_g, new_u), 0, CHUNK), shares(summed, 0, n, CHUNK), bufs[12:18])
    new_left = Rings(
        n, me, left, gu_part, dn_part, whole * CHUNK, columns((new_g, new_u), whole * CHUNK, left), shares(summed, whole * share, n, left), bufs[18:24]
    )
    tiles = tokens // TILE

    def tick(k):
        slot, s = lax.rem(k, 4), k // 4

        @pl.when((s < old.actions) & (slot < whole - early))
        def _():
            old.step(slot, s)

        @pl.when((s < old.actions) & (slot == 2))
        def _():
            old_left.step(0, s)

        rotate4(new, k, whole, tiles)

    prepare(tokens, h_ref, dh_ref, a, a_t, dh_t)
    ready = early * CHUNK
    sum_g[1, :, :ready] = old_sum_g[...]
    sum_u[1, :, :ready] = old_sum_u[...]
    old_summed[: early * share, :] = old_sum_d[...]
    refs = (dh_ref, gu, dn, a, a_t, dh_t, dn_t, None, acc_g, acc_u, acc_d)
    backward_layer(tokens, refs, placer(gu_part, dn_part), ff, None, tick)
    old_over = Handover(n, me, ff, old_summed, sum_d.at[1], old_send, old_recv)
    over = Handover(n, me, ff, summed, sum_d.at[0], send, recv)
    total = (whole + 1) * tiles

    def rest(i, _):
        @pl.when(lax.rem(i, 4) == 2)
        def _():
            new_left.step(0, i // 4)

        rotate4(new, total + i, whole, tiles)
        return 0

    lax.fori_loop(0, 4, rest, 0)
    old_over.start()
    lax.fori_loop(4, 4 * new.actions, rest, 0)
    over.start()
    old.end(whole - early)
    old_left.end(1)
    new.end(whole)
    new_left.end(1)
    old_over.end()
    over.end()


def work_scratch(tokens, d):
    return [
        pltpu.VMEM((tokens, d), BF16),
        pltpu.VMEM((d, tokens), BF16),
        pltpu.VMEM((d, tokens), BF16),
        pltpu.VMEM((d, CHUNK), BF16),
    ]


def sums_scratch(d):
    return [pltpu.VMEM((d, CHUNK), F32)] * 3


def backward_last(n, early, h, dh, gu, dn):
    tokens, d = h.shape
    ff = dn.shape[0]
    ready = early * CHUNK
    vmem = pl.BlockSpec(memory_space=pltpu.VMEM)
    gu_sum = jax.ShapeDtypeStruct((d // n, ready), BF16)
    return pl.pallas_call(
        functools.partial(last_kernel, n, early),
        out_shape=(
            jax.ShapeDtypeStruct((tokens, d), BF16),
            jax.ShapeDtypeStruct((2, d, ff - ready), BF16),
            jax.ShapeDtypeStruct((ff - ready, d), BF16),
            gu_sum, gu_sum, jax.ShapeDtypeStruct((ready // n, d), BF16),
        ),
        in_specs=[vmem] * 4,
        out_specs=(vmem,) * 6,
        scratch_shapes=work_scratch(tokens, d)
        + [pltpu.VMEM((2 * CHUNK, d), BF16)]
        + sums_scratch(d)
        + [pltpu.VMEM((tokens, d), F32), pltpu.VMEM((2, d, ff), BF16), pltpu.VMEM((ff, d), BF16)]
        + ring_scratch(n, early, CHUNK, d),
        compiler_params=pltpu.CompilerParams(collective_id=1, has_side_effects=True, vmem_limit_bytes=VMEM_LIMIT),
        name="layer1",
    )(h, dh, gu, dn)


def backward_first(n, early, h, dh, gu, dn, *old):
    tokens, d = h.shape
    ff = dn.shape[0]
    whole, left, units = ff // CHUNK, ff % CHUNK, ff // n // 16
    vmem = pl.BlockSpec(memory_space=pltpu.VMEM)
    gu_sum = jax.ShapeDtypeStruct((2, d // n, ff), BF16)
    sems = pltpu.SemaphoreType.DMA((units,))
    return pl.pallas_call(
        functools.partial(first_kernel, n, early),
        out_shape=(gu_sum, gu_sum, jax.ShapeDtypeStruct((2, units, 16, d), BF16)),
        in_specs=[vmem] * 9,
        out_specs=(vmem,) * 3,
        scratch_shapes=work_scratch(tokens, d)
        + sums_scratch(d)
        + [pltpu.VMEM((2, d, ff), BF16), pltpu.VMEM((ff, d), BF16)]
        + [pltpu.VMEM((ff // n, d), BF16)] * 2
        + [sems] * 4
        + ring_scratch(n, whole - early, CHUNK, d)
        + ring_scratch(n, 1, left, d)
        + ring_scratch(n, whole, CHUNK, d)
        + ring_scratch(n, 1, left, d),
        compiler_params=pltpu.CompilerParams(collective_id=2, has_side_effects=True, vmem_limit_bytes=VMEM_LIMIT),
        name="layer0",
    )(h, dh, gu, dn, *old)


def solution(mesh):
    n = mesh.shape["dp"]

    def step(x, dy, *arrays):
        weights, m, v = (arrays[i : i + 3] for i in (0, 3, 6))
        h1, gu0, d0, gu1, d1 = forward(n, x[0], *weights)
        by_h1, *old = backward_last(n, EARLY, h1, dy[0], gu1, d1)
        *sums, by_down = backward_first(n, EARLY, x[0], by_h1, gu0, d0, *old)
        gradients = [g.astype(F32) for g in (*sums, by_down.reshape(weights[2].shape))]
        new = [adamw(w.astype(F32), m, v, g) for w, m, v, g in zip(weights, m, v, gradients, strict=True)]
        return tuple(one[which] for which in range(3) for one in new)

    states, cut = P(("rep", "dp"), None, None), P(None, "dp", None)
    return jax.shard_map(
        step,
        mesh=mesh,
        in_specs=(states, states) + (cut,) * 9,
        out_specs=(P("rep", "dp", None),) * 9,
        check_vma=False,
    )
```

```python
import functools

import jax
import jax.numpy as jnp
from jax import lax
from jax.experimental import pallas as pl
from jax.experimental.pallas import tpu as pltpu
from jax.sharding import PartitionSpec as P

BF16, F32 = jnp.bfloat16, jnp.float32
MESH = pl.DeviceIdType.MESH
TILE = 512
CHUNK = 256
PIECES = 4
EARLY = 5
VMEM_LIMIT = 63 * 1024 * 1024


def dot(a, b):
    return jnp.dot(a, b, preferred_element_type=F32)


def scale_of(wide):
    return lax.rsqrt(jnp.mean(wide * wide, -1, keepdims=True) + 1e-6)


def sigmoid(g):
    return 0.5 * jnp.tanh(0.5 * g) + 0.5


def adamw(w, m, v, g):
    m = 0.9 * m + 0.1 * g
    v = 0.95 * v + 0.05 * g * g
    step = m * lax.rsqrt(v + 1e-8) + 0.1 * w
    return (w - 0.02 * step).astype(BF16), m, v


def tile_rows(t):
    return pl.ds(pl.multiple_of(t * TILE, TILE), TILE)


def greet(others):
    barrier = pltpu.get_barrier_semaphore()
    for other in others:
        pl.semaphore_signal(barrier, inc=1, device_id=other, device_id_type=MESH)
    pl.semaphore_wait(barrier, len(others))


def forward_kernel(
    n, x_ref, gate_ref, up_ref, down_ref, h_ref, gu0_out, d0_out, gu1_out, d1_out,
    gu, dn, hid, own_sem, out_sem, send_sem, recv_sem, psend_sem, precv_sem,
):
    me = lax.axis_index("dp")
    rep = lax.axis_index("rep")
    core = lax.rem(rep, 2)
    right, left = {"dp": lax.rem(me + 1, n)}, {"dp": lax.rem(me + n - 1, n)}
    partner = {"rep": rep + 1 - 2 * core}
    layers, rows, ff = gate_ref.shape
    drows, d = down_ref.shape[1:]
    half, quarter = d // 2, d // 4
    tiles = x_ref.shape[0] // TILE

    def own(l):
        mine = pl.ds(pl.multiple_of(me * rows, rows), rows)
        down = pl.ds(pl.multiple_of(me * drows, 16), drows)
        return (
            pltpu.make_async_copy(gate_ref.at[l], gu.at[l, 0, mine], own_sem.at[l, 0]),
            pltpu.make_async_copy(up_ref.at[l], gu.at[l, 1, mine], own_sem.at[l, 1]),
            pltpu.make_async_copy(down_ref.at[l], dn.at[l, down], own_sem.at[l, 2]),
        )

    for l in range(layers):
        for copy in own(l):
            copy.start()
    greet((right, left, partner))

    def piece(l, c, part, k):
        if part < 2:
            start = pl.multiple_of(k * rows + part * (rows // 2), rows // 2)
            return gu.at[l, c, pl.ds(start, rows // 2)]
        start = pl.multiple_of(k * drows, 16)
        return dn.at[l, pl.ds(start, drows), pl.ds(pl.multiple_of(c * half + (part - 2) * quarter, quarter), quarter)]

    def hops(side, part):
        return n // 2 if side == part % 2 else n - 1 - n // 2

    def ring(l, side, part, s, k):
        ref = piece(l, core, part, k)
        return pltpu.make_async_remote_copy(
            ref, ref, send_sem.at[l, side, part, s], recv_sem.at[l, side, part, s], (right, left)[side], MESH
        )

    def across(l, c, side, part, s, k):
        ref = piece(l, c, part, k)
        return pltpu.make_async_remote_copy(
            ref, ref, psend_sem.at[l, side, part, s], precv_sem.at[l, side, part, s], partner, MESH
        )

    def holder(side, s):
        return lax.rem(me + n - s, n) if side == 0 else lax.rem(me + s, n)

    def gather_step(l, s):
        for part in range(PIECES):
            for side in range(2):
                k, last = holder(side, s), hops(side, part)

                @pl.when((s > 0) & (s <= last))
                def _():
                    ring(l, side, part, s - 1, k).wait_recv()

                @pl.when(s < last)
                def _():
                    ring(l, side, part, s, k).start()

                @pl.when((s > 0) & (s <= last))
                def _():
                    across(l, core, side, part, s - 1, k).start()

    def gather_end(l):
        def body(s, _):
            for part in range(PIECES):
                for side in range(2):

                    @pl.when(s < hops(side, part))
                    def _():
                        k = holder(side, s + 1)
                        across(l, 1 - core, side, part, s, k).wait_recv()
                        across(l, core, side, part, s, k).wait_send()
                        ring(l, side, part, s, holder(side, s)).wait_send()

            return 0

        lax.fori_loop(0, n // 2, body, 0)

    def outs(l):
        to = ((gu0_out, d0_out), (gu1_out, d1_out))[l]
        return (
            pltpu.make_async_copy(gu.at[l], to[0], out_sem.at[l, 0]),
            pltpu.make_async_copy(dn.at[l], to[1], out_sem.at[l, 1]),
        )

    for l in range(layers):
        for copy in own(l):
            copy.wait()

    def gather_first(s, _):
        gather_step(0, s)

        @pl.when(s == n // 4)
        def _():
            gather_step(1, s - n // 4)

        return 0

    lax.fori_loop(0, n // 2 + 1, gather_first, 0)
    gather_end(0)
    for copy in outs(0):
        copy.start()

    def tile(t, _):
        @pl.when(lax.rem(t * (n // 2), tiles) < n // 2)
        def _():
            gather_step(1, 1 + t * (n // 2) // tiles)

        x = x_ref[tile_rows(t), :].astype(F32)
        a = (x * scale_of(x)).astype(BF16)
        for c in range(0, ff, CHUNK):
            w = min(CHUNK, ff - c)
            if w == CHUNK:
                g = dot(a, gu[0, 0, :, c : c + w])
                u = dot(a, gu[0, 1, :, c : c + w])
            else:
                both = dot(a, jnp.concatenate([gu[0, 0, :, c : c + w], gu[0, 1, :, c : c + w]], 1))
                g, u = both[:, :w], both[:, w:]
            hid[:, c : c + w] = (g * sigmoid(g) * u).astype(BF16)
        y = dot(hid[...], dn[0]).astype(BF16)
        h_ref[tile_rows(t), :] = (x + y.astype(F32)).astype(BF16)
        return 0

    lax.fori_loop(0, tiles, tile, 0)
    gather_end(1)
    for copy in outs(1):
        copy.start()
    for l in range(layers):
        for copy in outs(l):
            copy.wait()


def forward(n, x, gate, up, down):
    tokens, d = x.shape
    layers, rows, ff = gate.shape
    drows = down.shape[1]
    gu, dn = jax.ShapeDtypeStruct((2, d, ff), BF16), jax.ShapeDtypeStruct((n * drows, d), BF16)
    any_, vmem = pl.BlockSpec(memory_space=pl.ANY), pl.BlockSpec(memory_space=pltpu.VMEM)
    sems = pltpu.SemaphoreType.DMA((layers, 2, PIECES, n // 2))
    return pl.pallas_call(
        functools.partial(forward_kernel, n),
        out_shape=(jax.ShapeDtypeStruct(x.shape, BF16), gu, dn, gu, dn),
        in_specs=[vmem, any_, any_, any_],
        out_specs=(vmem, any_, any_, any_, any_),
        scratch_shapes=[
            pltpu.VMEM((layers, 2, d, ff), BF16),
            pltpu.VMEM((layers, n * drows, d), BF16),
            pltpu.VMEM((TILE, ff), BF16),
            pltpu.SemaphoreType.DMA((layers, 3)),
            pltpu.SemaphoreType.DMA((layers, 2)),
            sems, sems, sems, sems,
        ],
        compiler_params=pltpu.CompilerParams(collective_id=0, has_side_effects=True, vmem_limit_bytes=VMEM_LIMIT),
        name="gather_forward",
    )(x, gate, up, down)


class Rings:
    def __init__(self, n, me, w, gu, dn, base, out_gu, out_dn, bufs):
        self.n, self.me, self.w, self.gu, self.dn, self.base, self.out_gu, self.out_dn = n, me, w, gu, dn, base, out_gu, out_dn
        self.bufs = (bufs[0:3], bufs[3:6])
        self.rows = gu.shape[1] // n
        self.far = n // 2
        self.actions = self.far + 1

    def hops(self, kind, side):
        return self.far if side == kind else self.n - 1 - self.far

    def part(self, kind, j, k):
        first = self.base + j * self.w
        if kind == 0:
            first = first if isinstance(first, int) else pl.multiple_of(first, self.w)
            return self.gu.at[:, pl.ds(pl.multiple_of(k * self.rows, self.rows), self.rows), pl.ds(first, self.w)]
        share = self.w // self.n
        return self.dn.at[pl.ds(pl.multiple_of(first + k * share, share), share)]

    def at(self, kind, side, s):
        return s if side == 0 else self.hops(kind, 0) + s

    def copy(self, kind, j, side, src, s):
        slots, send, recv = self.bufs[kind]
        at = self.at(kind, side, s)
        to = lax.rem(self.me + (1 if side == 0 else self.n - 1), self.n)
        return pltpu.make_async_remote_copy(src, slots.at[j, at], send.at[j, at], recv.at[j, at], {"dp": to}, MESH)

    def slot(self, kind, j, side, s):
        return self.bufs[kind][0].at[j, self.at(kind, side, s)]

    def step(self, j, s):
        n, me = self.n, self.me

        def whose(kind, side, s):
            left = self.hops(kind, side) - s
            return lax.rem(me + left, n) if side == 0 else lax.rem(me + n - left, n)

        every = [(kind, side) for kind in range(2) for side in range(2)]

        @pl.when(s == 0)
        def _():
            for kind, side in every:
                self.copy(kind, j, side, self.part(kind, j, whose(kind, side, 0)), 0).start()

        @pl.when((s > 0) & (s < self.far))
        def _():
            for kind, side in every:

                @pl.when(s < self.hops(kind, side))
                def _():
                    here = self.slot(kind, j, side, s - 1)
                    self.copy(kind, j, side, here, s - 1).wait_recv()
                    term = self.part(kind, j, whose(kind, side, s))[...]
                    here[...] = (here[...].astype(F32) + term.astype(F32)).astype(BF16)
                    self.copy(kind, j, side, here, s).start()

        @pl.when(s == self.far)
        def _():
            for kind in range(2):
                total = self.part(kind, j, me)[...].astype(F32)
                for side in range(2):
                    here = self.slot(kind, j, side, self.hops(kind, side) - 1)
                    self.copy(kind, j, side, here, self.hops(kind, side) - 1).wait_recv()
                    total += here[...].astype(F32)
                total = total.astype(BF16)
                if kind == 0:
                    for p in range(2):
                        self.out_gu(p, j)[...] = total[p]
                else:
                    self.out_dn(j)[...] = total

    def end(self, count):
        def body(j, _):
            for kind in range(2):
                for side in range(2):
                    for s in range(self.hops(kind, side)):
                        self.copy(kind, j, side, self.slot(kind, j, side, s), s).wait_send()
            return 0

        lax.fori_loop(0, count, body, 0)


def ring_scratch(n, count, w, d):
    sems = pltpu.SemaphoreType.DMA((count, n - 1))
    return [
        pltpu.VMEM((count, n - 1, 2, d // n, w), BF16), sems, sems,
        pltpu.VMEM((count, n - 1, w // n, d), BF16), sems, sems,
    ]


def columns(ref, first, w):
    return lambda side, j: ref[side].at[:, pl.ds(first + j * w if isinstance(j, int) else pl.multiple_of(first + j * w, w), w)]


def shares(ref, first, n, w):
    return lambda j: ref.at[pl.ds(pl.multiple_of(first + j * (w // n), w // n), w // n)]


def rotate3(rings, k, count, tiles):
    for more in (0, 3):
        j = lax.rem(2 * k + 2, 3) + more
        since = k - tiles * (j + 1)

        @pl.when((j < count) & (since >= 0) & (since < 3 * rings.actions))
        def _():
            rings.step(j, since // 3)


def rotate4(rings, k, count, tiles):
    for more in (0, 4):
        j = lax.rem(k, 4) + more
        since = k - tiles * (j + 1) - lax.rem(k, 4)

        @pl.when((j < count) & (since >= 0) & (since < 4 * rings.actions))
        def _():
            rings.step(j, since // 4)


class Handover:
    def __init__(self, n, me, ff, summed, to, send, recv):
        self.n, self.me, self.summed, self.to, self.send, self.recv = n, me, summed, to, send, recv
        self.units, self.per = ff // 16 // n, CHUNK // n // 16
        self.whole = ff // CHUNK * (CHUNK // 16)

    def copy(self, i):
        n, me, per = self.n, self.me, self.per
        whole = ff_unit = (i // per) * (n * per) + me * per + i % per
        if i * n * 16 >= self.whole * 16:
            left = self.units - self.whole // n
            ff_unit = self.whole + me * left + (i - self.whole // n)
        del whole
        owner, slot = ff_unit // self.units, lax.rem(ff_unit, self.units)
        src, dst = self.summed.at[pl.ds(16 * i, 16)], self.to.at[slot]
        return owner, slot, pltpu.make_async_remote_copy(src, dst, self.send.at[i], self.recv.at[slot], {"dp": owner}, MESH)

    def start(self):
        for i in range(self.units):
            owner, slot, copy = self.copy(i)

            @pl.when(owner == self.me)
            def _():
                self.to[slot] = self.summed[16 * i : 16 * i + 16, :]

            @pl.when(owner != self.me)
            def _():
                copy.start()

    def end(self):
        for i in range(self.units):
            owner, _, copy = self.copy(i)

            @pl.when(owner != self.me)
            def _():
                copy.wait_send()

        def body(slot, _):
            unit = self.units * self.me + slot
            left = self.units - self.whole // self.n
            source = jnp.where(unit < self.whole, lax.rem(unit, self.n * self.per) // self.per, (unit - self.whole) // left)

            @pl.when(source != self.me)
            def _():
                ref = self.to.at[slot]
                pltpu.make_async_remote_copy(ref, ref, self.send.at[0], self.recv.at[slot], {"dp": source}, MESH).wait_recv()

            return 0

        lax.fori_loop(0, self.units, body, 0)


def prepare(tokens, h_ref, dh_ref, a, a_t, dh_t):
    def body(t, _):
        rows = tile_rows(t)
        wide = h_ref[rows, :].astype(F32)
        normed = (wide * scale_of(wide)).astype(BF16)
        a[rows, :] = normed
        a_t[:, rows] = normed.T
        dh_t[:, rows] = dh_ref[rows, :].T
        return 0

    lax.fori_loop(0, tokens // TILE, body, 0)


def backward_chunk(tokens, c, w, refs, place, da, tick):
    dh_ref, gu, dn, a, a_t, dh_t, dn_t, gu_t, acc_g, acc_u, acc_d = refs
    units = pl.ds(c if isinstance(c, int) else pl.multiple_of(c, CHUNK), w)
    dn_t[:, :w] = dn[units, :].T
    if da is not None:
        gu_t[:w] = gu[0, :, units].T
        gu_t[w : 2 * w] = gu[1, :, units].T
    acc_g[...] = jnp.zeros_like(acc_g)
    acc_u[...] = jnp.zeros_like(acc_u)
    acc_d[...] = jnp.zeros_like(acc_d)

    def body(t, _):
        tick(t)
        rows = tile_rows(t)
        at = a[rows, :]
        if w == CHUNK:
            g = dot(at, gu[0, :, units])
            u = dot(at, gu[1, :, units])
        else:
            both = dot(at, jnp.concatenate([gu[0, :, units], gu[1, :, units]], 1))
            g, u = both[:, :w], both[:, w:]
        e = dot(dh_ref[rows, :], dn_t[:, :w]).astype(BF16).astype(F32)
        s = sigmoid(g)
        silu = g * s
        hid = (silu * u).astype(BF16)
        du = (e * silu).astype(BF16)
        dg = (e * u * (s + silu * (1.0 - s))).astype(BF16)
        acc_d[:, :w] += dot(dh_t[:, rows], hid)
        dgu = jnp.concatenate([dg, du], 1)
        if w == CHUNK:
            acc_g[...] += dot(a_t[:, rows], dg)
            acc_u[...] += dot(a_t[:, rows], du)
        else:
            acc_g[...] += dot(a_t[:, rows], dgu)
        if da is not None:
            da[rows, :] += dot(dgu, gu_t[: 2 * w, :])
        return 0

    lax.fori_loop(0, tokens // TILE, body, 0)
    if w == CHUNK:
        place(acc_g[...], acc_u[...], acc_d[...])
    else:
        place(acc_g[:, :w], acc_g[:, w : 2 * w], acc_d[:, :w])


def backward_layer(tokens, refs, place, ff, da, tick):
    tiles = tokens // TILE
    whole = ff // CHUNK

    def chunk(j, _):
        c = pl.multiple_of(j * CHUNK, CHUNK)
        backward_chunk(tokens, c, CHUNK, refs, place(c, CHUNK), da, lambda t: tick(j * tiles + t))
        return 0

    lax.fori_loop(0, whole, chunk, 0)
    if ff % CHUNK:
        backward_chunk(tokens, whole * CHUNK, ff % CHUNK, refs, place(whole * CHUNK, ff % CHUNK), da, lambda t: tick(whole * tiles + t))


def placer(gu_part, dn_part):
    def place(c, w):
        def put(g, u, d):
            gu_part[0, :, pl.ds(c, w)] = g.astype(BF16)
            gu_part[1, :, pl.ds(c, w)] = u.astype(BF16)
            dn_part[pl.ds(c, w), :] = d.astype(BF16).T

        return put

    return place


def last_kernel(
    n, early, h_ref, dh_ref, gu, dn, out_h, out_gu, out_dn, sum_g, sum_u, sum_d,
    a, a_t, dh_t, dn_t, gu_t, acc_g, acc_u, acc_d, da, gu_part, dn_part, *bufs,
):
    me = lax.axis_index("dp")
    tokens, d = h_ref.shape
    ff = dn.shape[0]
    greet(({"dp": lax.rem(me + 1, n)}, {"dp": lax.rem(me + n - 1, n)}))
    rings = Rings(n, me, CHUNK, gu_part, dn_part, 0, columns((sum_g, sum_u), 0, CHUNK), shares(sum_d, 0, n, CHUNK), bufs)
    tiles = tokens // TILE
    prepare(tokens, h_ref, dh_ref, a, a_t, dh_t)
    da[...] = jnp.zeros_like(da)
    refs = (dh_ref, gu, dn, a, a_t, dh_t, dn_t, gu_t, acc_g, acc_u, acc_d)
    backward_layer(tokens, refs, placer(gu_part, dn_part), ff, da, lambda k: rotate3(rings, k, early, tiles))
    out_gu[...] = gu_part[:, :, early * CHUNK :]
    out_dn[...] = dn_part[early * CHUNK :, :]

    def finish(t, _):
        rows = tile_rows(t)
        wide = h_ref[rows, :].astype(F32)
        r = scale_of(wide)
        by_a = da[rows, :].astype(BF16).astype(F32)
        by_h = by_a * r - wide * (r * r * r * jnp.mean(by_a * wide, -1, keepdims=True))
        out_h[rows, :] = (dh_ref[rows, :].astype(F32) + by_h.astype(BF16).astype(F32)).astype(BF16)
        return 0

    lax.fori_loop(0, tiles, finish, 0)
    rings.end(early)


def first_kernel(
    n, early, h_ref, dh_ref, gu, dn, old_gu, old_dn, old_sum_g, old_sum_u, old_sum_d, sum_g, sum_u, sum_d,
    a, a_t, dh_t, dn_t, acc_g, acc_u, acc_d, gu_part, dn_part, summed, old_summed, send, recv, old_send, old_recv, *bufs,
):
    me = lax.axis_index("dp")
    tokens, d = h_ref.shape
    ff = dn.shape[0]
    whole, left = ff // CHUNK, ff % CHUNK
    share = CHUNK // n
    barrier = pltpu.get_barrier_semaphore()
    for other in range(1, n):
        pl.semaphore_signal(barrier, inc=1, device_id={"dp": lax.rem(me + other, n)}, device_id_type=MESH)
    pl.semaphore_wait(barrier, n - 1)
    old_g, old_u, new_g, new_u = sum_g.at[1], sum_u.at[1], sum_g.at[0], sum_u.at[0]
    old = Rings(
        n, me, CHUNK, old_gu, old_dn, 0, columns((old_g, old_u), early * CHUNK, CHUNK), shares(old_summed, early * share, n, CHUNK), bufs[0:6]
    )
    old_left = Rings(
        n, me, left, old_gu, old_dn, (whole - early) * CHUNK, columns((old_g, old_u), whole * CHUNK, left), shares(old_summed, whole * share, n, left), bufs[6:12]
    )
    new = Rings(n, me, CHUNK, gu_part, dn_part, 0, columns((new_g, new_u), 0, CHUNK), shares(summed, 0, n, CHUNK), bufs[12:18])
    new_left = Rings(
        n, me, left, gu_part, dn_part, whole * CHUNK, columns((new_g, new_u), whole * CHUNK, left), shares(summed, whole * share, n, left), bufs[18:24]
    )
    tiles = tokens // TILE

    def tick(k):
        slot, s = lax.rem(k, 4), k // 4

        @pl.when((s < old.actions) & (slot < whole - early))
        def _():
            old.step(slot, s)

        @pl.when((s < old.actions) & (slot == 2))
        def _():
            old_left.step(0, s)

        rotate4(new, k, whole, tiles)

    prepare(tokens, h_ref, dh_ref, a, a_t, dh_t)
    ready = early * CHUNK
    sum_g[1, :, :ready] = old_sum_g[...]
    sum_u[1, :, :ready] = old_sum_u[...]
    old_summed[: early * share, :] = old_sum_d[...]
    refs = (dh_ref, gu, dn, a, a_t, dh_t, dn_t, None, acc_g, acc_u, acc_d)
    backward_layer(tokens, refs, placer(gu_part, dn_part), ff, None, tick)
    old_over = Handover(n, me, ff, old_summed, sum_d.at[1], old_send, old_recv)
    over = Handover(n, me, ff, summed, sum_d.at[0], send, recv)
    total = (whole + 1) * tiles

    def rest(i, _):
        @pl.when(lax.rem(i, 4) == 2)
        def _():
            new_left.step(0, i // 4)

        rotate4(new, total + i, whole, tiles)
        return 0

    lax.fori_loop(0, 4, rest, 0)
    old_over.start()
    lax.fori_loop(4, 4 * new.actions, rest, 0)
    over.start()
    old.end(whole - early)
    old_left.end(1)
    new.end(whole)
    new_left.end(1)
    old_over.end()
    over.end()


def work_scratch(tokens, d):
    return [
        pltpu.VMEM((tokens, d), BF16),
        pltpu.VMEM((d, tokens), BF16),
        pltpu.VMEM((d, tokens), BF16),
        pltpu.VMEM((d, CHUNK), BF16),
    ]


def sums_scratch(d):
    return [pltpu.VMEM((d, CHUNK), F32)] * 3


def backward_last(n, early, h, dh, gu, dn):
    tokens, d = h.shape
    ff = dn.shape[0]
    ready = early * CHUNK
    vmem = pl.BlockSpec(memory_space=pltpu.VMEM)
    gu_sum = jax.ShapeDtypeStruct((d // n, ready), BF16)
    return pl.pallas_call(
        functools.partial(last_kernel, n, early),
        out_shape=(
            jax.ShapeDtypeStruct((tokens, d), BF16),
            jax.ShapeDtypeStruct((2, d, ff - ready), BF16),
            jax.ShapeDtypeStruct((ff - ready, d), BF16),
            gu_sum, gu_sum, jax.ShapeDtypeStruct((ready // n, d), BF16),
        ),
        in_specs=[vmem] * 4,
        out_specs=(vmem,) * 6,
        scratch_shapes=work_scratch(tokens, d)
        + [pltpu.VMEM((2 * CHUNK, d), BF16)]
        + sums_scratch(d)
        + [pltpu.VMEM((tokens, d), F32), pltpu.VMEM((2, d, ff), BF16), pltpu.VMEM((ff, d), BF16)]
        + ring_scratch(n, early, CHUNK, d),
        compiler_params=pltpu.CompilerParams(collective_id=1, has_side_effects=True, vmem_limit_bytes=VMEM_LIMIT),
        name="layer1",
    )(h, dh, gu, dn)


def backward_first(n, early, h, dh, gu, dn, *old):
    tokens, d = h.shape
    ff = dn.shape[0]
    whole, left, units = ff // CHUNK, ff % CHUNK, ff // n // 16
    vmem = pl.BlockSpec(memory_space=pltpu.VMEM)
    gu_sum = jax.ShapeDtypeStruct((2, d // n, ff), BF16)
    sems = pltpu.SemaphoreType.DMA((units,))
    return pl.pallas_call(
        functools.partial(first_kernel, n, early),
        out_shape=(gu_sum, gu_sum, jax.ShapeDtypeStruct((2, units, 16, d), BF16)),
        in_specs=[vmem] * 9,
        out_specs=(vmem,) * 3,
        scratch_shapes=work_scratch(tokens, d)
        + sums_scratch(d)
        + [pltpu.VMEM((2, d, ff), BF16), pltpu.VMEM((ff, d), BF16)]
        + [pltpu.VMEM((ff // n, d), BF16)] * 2
        + [sems] * 4
        + ring_scratch(n, whole - early, CHUNK, d)
        + ring_scratch(n, 1, left, d)
        + ring_scratch(n, whole, CHUNK, d)
        + ring_scratch(n, 1, left, d),
        compiler_params=pltpu.CompilerParams(collective_id=2, has_side_effects=True, vmem_limit_bytes=VMEM_LIMIT),
        name="layer0",
    )(h, dh, gu, dn, *old)


def solution(mesh):
    n = mesh.shape["dp"]

    def step(x, dy, *arrays):
        weights, m, v = (arrays[i : i + 3] for i in (0, 3, 6))
        h1, gu0, d0, gu1, d1 = forward(n, x[0], *weights)
        by_h1, *old = backward_last(n, EARLY, h1, dy[0], gu1, d1)
        *sums, by_down = backward_first(n, EARLY, x[0], by_h1, gu0, d0, *old)
        gradients = [g.astype(F32) for g in (*sums, by_down.reshape(weights[2].shape))]
        new = [adamw(w.astype(F32), m, v, g) for w, m, v, g in zip(weights, m, v, gradients, strict=True)]
        return tuple(one[which] for which in range(3) for one in new)

    states, cut = P(("rep", "dp"), None, None), P(None, "dp", None)
    return jax.shard_map(
        step,
        mesh=mesh,
        in_specs=(states, states) + (cut,) * 9,
        out_specs=(P("rep", "dp", None),) * 9,
        check_vma=False,
    )
```
